32 devices in a mesh: tm: 4 (over z), env: 8 (over y, x, core).
Axes of the slice: x: 2, y: 2, z: 4, core: 2. Of those that a mesh axis runs over, the one named last changes fastest.
Arguments:
- rewards: float32 [1024, 1024], P('tm', 'env'), may hold values from -6 to 6
- dones: int32 [1024, 1024], P('tm', 'env'), may hold values 0 or 1
- horizon: float32 [1024], P('env'), may hold values from 20 to 2048
- bootstrap: float32 [1024], P('env'), may hold values from -96 to 96
- prior_mean: float32 [1], replicated, may hold values from -240 to 240
- prior_var: float32 [1], replicated, may hold values from 100 to 3000
Outputs:
- scaled_rewards: float32 [1024, 1024], P('tm', 'env')
- scaled_returns: float32 [1024, 1024], P('tm', 'env')
- running_stats: float32 [2], replicated
The draws below stay inside these ranges and needn't reach their ends.
All inputs are finite; a program needn't handle non-finite values. No bound on the sum of `dones` on one device may be relied on, other than what follows from the above.
Results may differ from the reference program's by a relative error of at most 0.0003.
Values sent between devices are 32-bit elements; how exact they have to be, the bound alone decides.
A program may use at most 64 MiB of HBM per device.

```python
import math
import jax
import jax.numpy as jnp
from jax import lax

TIME = 1024
ENVS = 1024
PRIOR = 1048576


def place_ends(result, key, least, largest):
    place = [jax.random.randint(jax.random.fold_in(key, axis), (), 0, length) for axis, length in enumerate(result.shape)]
    widest = result.shape.index(max(result.shape))
    beside = place[:widest] + [(place[widest] + 1) % result.shape[widest]] + place[widest + 1:]
    return result.at[tuple(place)].set(least).at[tuple(beside)].set(largest)


def level_of(rng, shape, pieces, low, largest):
    def one(dim, parts):
        steps = jax.random.uniform(jax.random.fold_in(jax.random.fold_in(rng, 6), dim), (parts,), jnp.float32, low / len(pieces), largest / len(pieces))
        return jnp.repeat(jnp.exp(steps), shape[dim] // parts).reshape((-1,) + (1,) * (len(shape) - dim - 1))

    loudness = one(*pieces[0])
    for cut in pieces[1:]:
        loudness = loudness * one(*cut)
    return loudness


def bell_draw(stream_key, extent, scale, reach, pieces=(), kind=jnp.bfloat16):
    drawn = jax.random.normal(stream_key, extent, jnp.float32) * scale
    if len(pieces) > 0:
        drawn = level_of(stream_key, extent, pieces, -0.22, 0.18) * drawn
    return jnp.clip(drawn, min=-reach, max=reach).astype(kind)


def setup_inputs(seed: int = 0) -> dict:
    arg_keys = jax.random.split(jax.random.key(seed), 7)
    rewards = bell_draw(arg_keys[0], (TIME, ENVS), 1.0, 6.0, ((0, 4), (1, 8)), jnp.float32)
    dones = place_ends((jax.random.randint(arg_keys[1], (TIME, ENVS), 0, 4 * TIME) < 1).astype(jnp.int32), jax.random.fold_in(arg_keys[1], 1), 0, 1)
    horizon = jnp.clip(jnp.exp(math.log(2048.0) - 4.6288867 * jax.random.uniform(arg_keys[2], (ENVS,), jnp.float32) ** level_of(arg_keys[2], (ENVS,), ((0, 8),), -0.2, 0.2)), 20.0, 2048.0)
    bootstrap = bell_draw(arg_keys[3], (ENVS,), 16.0, 96.0, ((0, 8),), jnp.float32)
    prior_mean = bell_draw(arg_keys[4], (1,), 40.0, 240.0, (), jnp.float32)
    prior_var = jnp.clip(jnp.exp(jax.random.uniform(arg_keys[5], (1,), jnp.float32, math.log(100.0), math.log(3000.0))), 100.0, 3000.0)
    return {"rewards": rewards, "dones": dones, "horizon": horizon, "bootstrap": bootstrap, "prior_mean": prior_mean, "prior_var": prior_var}


def reference(rewards, dones, horizon, bootstrap, prior_mean, prior_var):
    discount = 1.0 - 1.0 / horizon
    factor = discount[None, :] * (1.0 - dones.astype(jnp.float32))

    def backward(carried, inputs):
        reward_row, factor_row = inputs
        updated = reward_row + factor_row * carried
        return (updated, updated)
    final_carry, returns = lax.scan(backward, bootstrap, (rewards, factor), reverse=True)
    entries = jnp.float32(returns.size)
    average = jnp.sum(returns) / entries
    spread = jnp.sum((returns - average) * (returns - average))
    prior_count = jnp.float32(PRIOR)
    merged = prior_count + entries
    delta = average - prior_mean[0]
    new_mean = prior_mean[0] + delta * entries / merged
    new_spread = prior_var[0] * prior_count + spread + delta * delta * prior_count * entries / merged
    variance = new_spread / merged
    inverse = 1.0 / jnp.sqrt(variance + 1e-08)
    return (rewards * inverse, returns * inverse, jnp.stack([new_mean, variance]))
```

```python
import functools

import jax
import jax.numpy as jnp
from jax import lax
from jax.experimental import pallas as pl
from jax.experimental.pallas import tpu as pltpu
from jax.sharding import PartitionSpec as P

SUB = 8
ROWS = 8
PARTS = 2


def compose_rows(summed, product, row):
    step = 1
    while step < SUB:
        inside = row < SUB - step
        later_sum = jnp.where(inside, pltpu.roll(summed, SUB - step, 0), 0.0)
        later_product = jnp.where(inside, pltpu.roll(product, SUB - step, 0), 1.0)
        summed = summed + product * later_sum
        product = product * later_product
        step *= 2
    return summed, product


def kernel(T, E, rewards_hbm, dones_hbm, horizon_hbm, bootstrap_hbm, prior,
           rewards, s_buf, p_buf, carry_ref, ebuf, prior_ref,
           dones, horizon_ref, bootstrap_ref, tbuf, xbuf,
           load_sem, small_sem, send_sem, recv_sem):
    t = lax.axis_index("tm")
    e = lax.axis_index("env")
    me = t * E + e
    peers = [k + jnp.where(k >= me, 1, 0) for k in range(T * E - 1)]
    loads = [pltpu.make_async_copy(rewards_hbm, rewards, load_sem.at[0]),
             pltpu.make_async_copy(dones_hbm, dones, load_sem.at[1])]
    smalls = [pltpu.make_async_copy(horizon_hbm, horizon_ref, small_sem.at[0]),
              pltpu.make_async_copy(bootstrap_hbm, bootstrap_ref, small_sem.at[1])]
    for load in smalls[:1] + loads + smalls[1:]:
        load.start()
    barrier = pltpu.get_barrier_semaphore()
    for peer in peers:
        pl.semaphore_signal(barrier, inc=1, device_id=peer, device_id_type=pl.DeviceIdType.LOGICAL)
    rows, lanes = rewards.shape
    chunk = rows // SUB
    shape = (SUB, lanes)
    row = lax.broadcasted_iota(jnp.int32, shape, 0)
    smalls[0].wait()
    discount = jnp.broadcast_to(1.0 - 1.0 / horizon_ref[...], shape)
    for load in loads:
        load.wait()
    s = jnp.zeros(shape, jnp.float32)
    p = jnp.ones(shape, jnp.float32)
    zero = jnp.zeros(shape, jnp.float32)
    s1, p1, s2, sp, p2 = zero, zero, zero, zero, zero
    for k in reversed(range(chunk)):
        r = rewards[pl.ds(k, SUB, stride=chunk), :]
        f = jnp.where(dones[pl.ds(k, SUB, stride=chunk), :] == 0, discount, 0.0)
        s = r + f * s
        p = f * p
        s_buf[k] = s
        p_buf[k] = p
        s1 = s1 + s
        p1 = p1 + p
        s2 = s2 + s * s
        sp = sp + s * p
        p2 = p2 + p * p
    full_s, full_p = compose_rows(s, p, row)
    last = row == SUB - 1
    a = jnp.where(last, 0.0, pltpu.roll(full_s, SUB - 1, 0))
    b = jnp.where(last, 1.0, pltpu.roll(full_p, SUB - 1, 0))
    down = lambda value: jnp.sum(value, axis=0, keepdims=True)
    smalls[1].wait()
    known = jnp.where(t == T - 1, bootstrap_ref[...], jnp.zeros((1, lanes), jnp.float32))
    a = a + b * known
    rest = sp + a * p2
    tbuf[me, 0:1] = full_s[0:1] + full_p[0:1] * known
    tbuf[me, 1:2] = full_p[0:1]
    tbuf[me, 2:3] = down(s1 + p1 * a)
    tbuf[me, 3:4] = down(p1 * b)
    tbuf[me, 4:5] = down(s2 + a * (sp + rest))
    tbuf[me, 5:6] = down(2.0 * b * rest)
    tbuf[me, 6:7] = down(b * b * p2)
    tbuf[me, 7:8] = prior[...]
    pl.semaphore_wait(barrier, T * E - 1)
    for peer in peers:
        pltpu.make_async_remote_copy(
            tbuf.at[me], tbuf.at[me], send_sem, recv_sem,
            device_id=peer, device_id_type=pl.DeviceIdType.LOGICAL).start()
    every = tbuf.at[0:T * E - 1]
    pltpu.make_async_copy(every, every, recv_sem).wait()
    x = jnp.zeros((E, lanes), jnp.float32)
    first = jnp.zeros((E, lanes), jnp.float32)
    second = jnp.zeros((E, lanes), jnp.float32)
    for j in reversed(range(T)):
        xbuf[j] = x
        part = pl.ds(j * E, E)
        first = first + tbuf[part, 2] + tbuf[part, 3] * x
        second = second + tbuf[part, 4] + x * (tbuf[part, 5] + x * tbuf[part, 6])
        x = tbuf[part, 0] + tbuf[part, 1] * x
    mine = xbuf[t, pl.ds(e, 1), :]
    prior_ref[...] = tbuf[0, 7:8]
    ebuf[0] = first
    ebuf[1] = second
    carry_ref[...] = a + b * mine
    pltpu.make_async_copy(every, every, send_sem).wait()


def pair_priors(mean, var, out):
    lane = lax.broadcasted_iota(jnp.int32, out.shape, 1)
    out[...] = jnp.where(lane == 0, mean[0], jnp.where(lane == out.shape[1] // 2, var[0], 0.0))


def finish(T, E, rewards, s_buf, p_buf, carry_ref, ebuf, prior_ref, out_rewards, out_returns, out_stats,
           rewards_out, returns_out, stats, sems):
    rows, lanes = rewards.shape
    chunk = rows // SUB
    entries = float(rows * T * lanes * E)
    prior_count = entries
    merged = prior_count + entries
    prior = prior_ref[...]
    is_mean = lax.broadcasted_iota(jnp.int32, prior.shape, 1) < lanes // 2
    first = jnp.sum(ebuf[0], axis=0, keepdims=True) * (1.0 / entries)
    second = jnp.sum(ebuf[1], axis=0, keepdims=True) * (1.0 / merged)
    across = lambda value: jnp.sum(value, axis=1, keepdims=True)
    average = across(first)
    delta = across(first - jnp.where(is_mean, prior, 0.0))
    squares = across(second + jnp.where(is_mean, 0.0, prior * (prior_count / merged)))
    new_mean = average - delta * (prior_count / merged)
    variance = (squares - average * average * (entries / merged)
                + delta * delta * (prior_count / merged * (entries / merged)))
    inverse = jnp.broadcast_to(lax.rsqrt(variance + 1e-08), (SUB, lanes))
    copies = []

    def send(source, target, rank):
        copy = pltpu.make_async_copy(source, target, sems.at[rank])
        copy.start()
        copies.append(copy)

    y = carry_ref[...] * inverse
    for k in range(chunk):
        returns_out[pl.ds(k, SUB, stride=chunk), :] = s_buf[k] * inverse + p_buf[k] * y
    send(returns_out, out_returns, 0)
    part = rows // PARTS
    for i in range(PARTS):
        for k in range(i * part, (i + 1) * part, SUB):
            rewards_out[k:k + SUB] = rewards[k:k + SUB] * inverse
        where = pl.ds(i * part, part)
        send(rewards_out.at[where], out_rewards.at[where], 2 + i)
    stats[0] = new_mean[0, 0]
    stats[1] = variance[0, 0]
    send(stats, out_stats, 1)
    for copy in copies:
        copy.wait()


def local(T, E, rewards, dones, horizon, bootstrap, prior_mean, prior_var):
    rows, lanes = rewards.shape
    block = (rows, lanes)
    vmem = pl.BlockSpec(memory_space=pltpu.VMEM)
    hbm = pl.BlockSpec(memory_space=pltpu.HBM)
    shapes = (block, (rows // SUB, SUB, lanes), (rows // SUB, SUB, lanes), (SUB, lanes), (2, E, lanes), (1, lanes))
    exchange = pl.pallas_call(
        functools.partial(kernel, T, E),
        out_shape=tuple(pltpu.VMEM(shape, jnp.float32) for shape in shapes),
        in_specs=[hbm] * 4 + [vmem],
        out_specs=(vmem,) * 6,
        scratch_shapes=[
            pltpu.VMEM(block, jnp.int32),
            pltpu.VMEM((1, lanes), jnp.float32),
            pltpu.VMEM((1, lanes), jnp.float32),
            pltpu.VMEM((T * E, ROWS, lanes), jnp.float32),
            pltpu.VMEM((T, E, lanes), jnp.float32),
            pltpu.SemaphoreType.DMA((2,)),
            pltpu.SemaphoreType.DMA((2,)),
            pltpu.SemaphoreType.DMA,
            pltpu.SemaphoreType.DMA,
        ],
        compiler_params=pltpu.CompilerParams(collective_id=0, has_side_effects=True),
    )
    smem = pl.BlockSpec(memory_space=pltpu.SMEM)
    pair = pl.pallas_call(
        pair_priors, out_shape=jax.ShapeDtypeStruct((1, lanes), jnp.float32),
        in_specs=[smem] * 2, out_specs=vmem)
    prior = lax.cond(lax.axis_index("tm") + lax.axis_index("env") == 0, pair,
                     lambda *_: jnp.zeros((1, lanes), jnp.float32), prior_mean, prior_var)
    between = exchange(rewards, dones, horizon.reshape(1, lanes), bootstrap.reshape(1, lanes), prior)
    return pl.pallas_call(
        functools.partial(finish, T, E),
        out_shape=(jax.ShapeDtypeStruct(block, jnp.float32),
                   jax.ShapeDtypeStruct(block, jnp.float32),
                   jax.ShapeDtypeStruct((2,), jnp.float32)),
        in_specs=[vmem] * 6,
        out_specs=(hbm, hbm, hbm),
        scratch_shapes=[
            pltpu.VMEM(block, jnp.float32),
            pltpu.VMEM(block, jnp.float32),
            pltpu.SMEM((2,), jnp.float32),
            pltpu.SemaphoreType.DMA((2 + PARTS,)),
        ],
        compiler_params=pltpu.CompilerParams(vmem_limit_bytes=4 * 2**20),
    )(*between)


def solution(mesh):
    T, E = mesh.shape["tm"], mesh.shape["env"]
    return jax.shard_map(
        functools.partial(local, T, E),
        mesh=mesh,
        in_specs=(P("tm", "env"), P("tm", "env"), P("env"), P("env"), P(), P()),
        out_specs=(P("tm", "env"), P("tm", "env"), P()),
        check_vma=False,
    )
```

```python
import functools

import jax
import jax.numpy as jnp
from jax import lax
from jax.experimental import pallas as pl
from jax.experimental.pallas import tpu as pltpu
from jax.sharding import PartitionSpec as P

SUB = 8
ROWS = 8


def compose_rows(summed, product, row):
    step = 1
    while step < SUB:
        inside = row < SUB - step
        later_sum = jnp.where(inside, pltpu.roll(summed, SUB - step, 0), 0.0)
        later_product = jnp.where(inside, pltpu.roll(product, SUB - step, 0), 1.0)
        summed = summed + product * later_sum
        product = product * later_product
        step *= 2
    return summed, product


def kernel(T, E, rewards_hbm, dones_hbm, horizon_hbm, bootstrap_hbm, prior,
           rewards, s_buf, p_buf, carry_ref, ebuf, prior_ref,
           dones, horizon_ref, bootstrap_ref, tbuf, xbuf, measure,
           load_sem, small_sem, send_sem, recv_sem):
    t = lax.axis_index("tm")
    e = lax.axis_index("env")
    me = t * E + e
    peers = [k + jnp.where(k >= me, 1, 0) for k in range(T * E - 1)]
    pieces = [pltpu.make_async_copy(source.at[i], target.at[:, i], load_sem.at[j])
              for j, (source, target) in enumerate(((rewards_hbm, rewards), (dones_hbm, dones)))
              for i in range(SUB)]
    loads = [pltpu.make_async_copy(target, target, load_sem.at[j]) for j, target in enumerate((rewards, dones))]
    smalls = [pltpu.make_async_copy(horizon_hbm, horizon_ref, small_sem.at[0]),
              pltpu.make_async_copy(bootstrap_hbm, bootstrap_ref, small_sem.at[1])]
    for load in smalls[:1] + pieces + smalls[1:]:
        load.start()
    barrier = pltpu.get_barrier_semaphore()
    for peer in reversed(peers):
        pl.semaphore_signal(barrier, inc=1, device_id=peer, device_id_type=pl.DeviceIdType.LOGICAL)
    chunk, _, lanes = rewards.shape
    shape = (SUB, lanes)
    row = lax.broadcasted_iota(jnp.int32, shape, 0)
    smalls[0].wait()
    discount = jnp.broadcast_to(1.0 - 1.0 / horizon_ref[...], shape)
    for load in loads:
        load.wait()
    s = jnp.zeros(shape, jnp.float32)
    p = jnp.ones(shape, jnp.float32)
    zero = jnp.zeros(shape, jnp.float32)
    s1, p1, s2, sp, p2 = zero, zero, zero, zero, zero
    for k in reversed(range(chunk)):
        r = rewards[k]
        f = jnp.where(dones[k] == 0, discount, 0.0)
        s = r + f * s
        p = f * p
        s_buf[k] = s
        p_buf[k] = p
        s1 = s1 + s
        p1 = p1 + p
        s2 = s2 + s * s
        sp = sp + s * p
        p2 = p2 + p * p
    full_s, full_p = compose_rows(s, p, row)
    last = row == SUB - 1
    a = jnp.where(last, 0.0, pltpu.roll(full_s, SUB - 1, 0))
    b = jnp.where(last, 1.0, pltpu.roll(full_p, SUB - 1, 0))
    down = lambda value: jnp.sum(value, axis=0, keepdims=True)
    smalls[1].wait()
    known = jnp.where(t == T - 1, bootstrap_ref[...], jnp.zeros((1, lanes), jnp.float32))
    a = a + b * known
    rest = sp + a * p2
    fold = lambda value: value + pltpu.roll(value, lanes // 2, 1)
    half = lax.broadcasted_iota(jnp.int32, (1, lanes), 1) < lanes // 2
    leading = full_s[0:1] + full_p[0:1] * known
    tbuf[me, 0:1] = jnp.where(half, fold(down(s1 + p1 * a)), fold(down(s2 + a * (sp + rest))))

    @pl.when(t == T - 1)
    def _():
        tbuf[me, 1:2] = leading

    @pl.when(t < T - 1)
    def _():
        tbuf[me, 1:2] = down(p1 * b)
        tbuf[me, 2:3] = down(2.0 * b * rest)
        tbuf[me, 3:4] = down(b * b * p2)
        tbuf[me, 4:5] = leading
        tbuf[me, 5:6] = full_p[0:1]
        tbuf[me, 6:7] = prior[...]

    pl.semaphore_wait(barrier, T * E - 1)
    total = E * sum(rows_sent(T, j) for j in range(T))
    for count in sorted({rows_sent(T, j) for j in range(T)}):
        blocks = [j for j in range(T) if rows_sent(T, j) == count]

        @pl.when(jnp.logical_and(t >= blocks[0], t <= blocks[-1]))
        def _():
            for peer in peers:
                pltpu.make_async_remote_copy(
                    tbuf.at[me, 0:count], tbuf.at[me, 0:count], send_sem, recv_sem,
                    device_id=peer, device_id_type=pl.DeviceIdType.LOGICAL).start()
            arrived = measure.at[0:total - count]
            pltpu.make_async_copy(arrived, arrived, recv_sem).wait()
            left = measure.at[0:(T * E - 1) * count]
            pltpu.make_async_copy(left, left, send_sem).wait()

    packed = jnp.zeros((E, lanes), jnp.float32)
    first = jnp.zeros((E, lanes), jnp.float32)
    second = jnp.zeros((E, lanes), jnp.float32)
    x = jnp.zeros((E, lanes), jnp.float32)
    for j in reversed(range(T)):
        part = pl.ds(j * E, E)
        xbuf[j] = x
        packed = packed + tbuf[part, 0]
        if j == T - 1:
            x = tbuf[part, 1]
            continue
        first = first + tbuf[part, 1] * x
        second = second + x * (tbuf[part, 2] + x * tbuf[part, 3])
        if j:
            x = tbuf[part, 4] + tbuf[part, 5] * x
    mine = xbuf[t, pl.ds(e, 1), :]
    prior_ref[0:1] = tbuf[reader(T, E), 6:7]
    prior_ref[1:2] = tbuf[reader(T, E) + 1, 6:7]
    ebuf[0] = packed
    ebuf[1] = first
    ebuf[2] = second
    carry_ref[...] = a + b * mine


def rows_sent(T, block):
    if block >= T - 2:
        return 2 if block == T - 1 else 7
    return 6 if block else 4


def reader(T, E):
    return max((T - 1) * E - 2, 0)


def pick(value, out):
    lane = lax.broadcasted_iota(jnp.int32, out.shape, 1)
    out[...] = jnp.where(lane == 0, value[0], 0.0)


def finish(T, E, rewards, s_buf, p_buf, carry_ref, ebuf, prior_ref, out_rewards, out_returns, out_stats,
           rewards_out, returns_out, stats, sems):
    chunk, _, lanes = rewards.shape
    entries = float(chunk * SUB * T * lanes * E)
    prior_count = entries
    half = lax.broadcasted_iota(jnp.int32, (1, lanes), 1) < lanes // 2
    merged = prior_count + entries
    down = lambda value: jnp.sum(value, axis=0, keepdims=True)
    packed = down(ebuf[0])
    first = (down(ebuf[1]) + jnp.where(half, packed, 0.0)) * (1.0 / entries)
    second = (down(ebuf[2]) + jnp.where(half, 0.0, packed)) * (1.0 / merged)
    across = lambda value: jnp.sum(value, axis=1, keepdims=True)
    average = across(first)
    delta = across(first - prior_ref[0:1])
    squares = across(second + prior_ref[1:2] * (prior_count / merged))
    new_mean = average - delta * (prior_count / merged)
    variance = (squares - average * average * (entries / merged)
                + delta * delta * (prior_count / merged * (entries / merged)))
    inverse = jnp.broadcast_to(lax.rsqrt(variance + 1e-08), (SUB, lanes))

    def send(source, target, rank):
        for i in range(SUB):
            pltpu.make_async_copy(source.at[:, i], target.at[i], sems.at[rank]).start()

    y = carry_ref[...] * inverse
    for k in range(chunk):
        returns_out[k] = s_buf[k] * inverse + p_buf[k] * y
    send(returns_out, out_returns, 0)
    for k in range(chunk):
        rewards_out[k] = rewards[k] * inverse
    send(rewards_out, out_rewards, 1)
    stats[0] = new_mean[0, 0]
    stats[1] = variance[0, 0]
    last = pltpu.make_async_copy(stats, out_stats, sems.at[2])
    last.start()
    pltpu.make_async_copy(returns_out, returns_out, sems.at[0]).wait()
    pltpu.make_async_copy(rewards_out, rewards_out, sems.at[1]).wait()
    last.wait()


def local(T, E, rewards, dones, horizon, bootstrap, prior_mean, prior_var):
    rows, lanes = rewards.shape
    split = (SUB, rows // SUB, lanes)
    vmem = pl.BlockSpec(memory_space=pltpu.VMEM)
    hbm = pl.BlockSpec(memory_space=pltpu.HBM)
    steps = (rows // SUB, SUB, lanes)
    shapes = (steps, steps, steps, (SUB, lanes), (3, E, lanes), (2, lanes))
    exchange = pl.pallas_call(
        functools.partial(kernel, T, E),
        out_shape=tuple(pltpu.VMEM(shape, jnp.float32) for shape in shapes),
        in_specs=[hbm] * 4 + [vmem],
        out_specs=(vmem,) * 6,
        scratch_shapes=[
            pltpu.VMEM(steps, jnp.int32),
            pltpu.VMEM((1, lanes), jnp.float32),
            pltpu.VMEM((1, lanes), jnp.float32),
            pltpu.VMEM((T * E, ROWS, lanes), jnp.float32),
            pltpu.VMEM((T, E, lanes), jnp.float32),
            pltpu.VMEM((T * E * ROWS, lanes), jnp.float32),
            pltpu.SemaphoreType.DMA((2,)),
            pltpu.SemaphoreType.DMA((2,)),
            pltpu.SemaphoreType.DMA,
            pltpu.SemaphoreType.DMA,
        ],
        compiler_params=pltpu.CompilerParams(collective_id=0, has_side_effects=True),
    )
    smem = pl.BlockSpec(memory_space=pltpu.SMEM)
    alone = pl.pallas_call(
        pick, out_shape=jax.ShapeDtypeStruct((1, lanes), jnp.float32), in_specs=[smem], out_specs=vmem)
    me = lax.axis_index("tm") * E + lax.axis_index("env")
    prior = lax.switch(
        jnp.clip(me - reader(T, E) + 1, 0, 3),
        (lambda *_: jnp.zeros((1, lanes), jnp.float32), lambda mean, _: alone(mean), lambda _, var: alone(var),
         lambda *_: jnp.zeros((1, lanes), jnp.float32)), prior_mean, prior_var)
    between = exchange(rewards.reshape(split), dones.reshape(split), horizon.reshape(1, lanes), bootstrap.reshape(1, lanes), prior)
    scaled_rewards, scaled_returns, stats = pl.pallas_call(
        functools.partial(finish, T, E),
        out_shape=(jax.ShapeDtypeStruct(split, jnp.float32),
                   jax.ShapeDtypeStruct(split, jnp.float32),
                   jax.ShapeDtypeStruct((2,), jnp.float32)),
        in_specs=[vmem] * 6,
        out_specs=(hbm, hbm, hbm),
        scratch_shapes=[
            pltpu.VMEM(steps, jnp.float32),
            pltpu.VMEM(steps, jnp.float32),
            pltpu.SMEM((2,), jnp.float32),
            pltpu.SemaphoreType.DMA((3,)),
        ],
        compiler_params=pltpu.CompilerParams(vmem_limit_bytes=4 * 2**20),
    )(*between)
    return scaled_rewards.reshape(rows, lanes), scaled_returns.reshape(rows, lanes), stats


def solution(mesh):
    T, E = mesh.shape["tm"], mesh.shape["env"]
    return jax.shard_map(
        functools.partial(local, T, E),
        mesh=mesh,
        in_specs=(P("tm", "env"), P("tm", "env"), P("env"), P("env"), P(), P()),
        out_specs=(P("tm", "env"), P("tm", "env"), P()),
        check_vma=False,
    )
```

```python
import functools

import jax
import jax.numpy as jnp
from jax import lax
from jax.experimental import pallas as pl
from jax.experimental.pallas import tpu as pltpu
from jax.sharding import PartitionSpec as P

SUB = 8
ROWS = 8


def compose_rows(summed, product, row):
    step = 1
    while step < SUB:
        inside = row < SUB - step
        later_sum = jnp.where(inside, pltpu.roll(summed, SUB - step, 0), 0.0)
        later_product = jnp.where(inside, pltpu.roll(product, SUB - step, 0), 1.0)
        summed = summed + product * later_sum
        product = product * later_product
        step *= 2
    return summed, product


def kernel(T, E, rewards_hbm, dones_hbm, horizon_hbm, bootstrap_hbm, prior,
           rewards, s_buf, p_buf, carry_ref, ebuf, prior_ref,
           dones, horizon_ref, bootstrap_ref, tbuf, xbuf, measure,
           load_sem, send_sem, recv_sem):
    t = lax.axis_index("tm")
    e = lax.axis_index("env")
    me = t * E + e
    peers = [k + jnp.where(k >= me, 1, 0) for k in range(T * E - 1)]
    chunk, _, lanes = rewards.shape
    pltpu.make_async_copy(horizon_hbm, horizon_ref, load_sem).start()
    pltpu.make_async_copy(bootstrap_hbm, bootstrap_ref, load_sem).start()
    for source, target in ((rewards_hbm, rewards), (dones_hbm, dones)):
        for i in range(SUB):
            pltpu.make_async_copy(source.at[i], target.at[:, i], load_sem).start()
    barrier = pltpu.get_barrier_semaphore()
    def greet(peer):
        pl.semaphore_signal(barrier, inc=1, device_id=peer, device_id_type=pl.DeviceIdType.LOGICAL)

    lax.fori_loop(0, T * E - 1 - me, lambda i, _: greet(T * E - 1 - i), None)
    lax.fori_loop(0, me, lambda i, _: greet(me - 1 - i), None)
    shape = (SUB, lanes)
    row = lax.broadcasted_iota(jnp.int32, shape, 0)
    loaded = measure.at[0:2 * chunk * SUB + 2]
    pltpu.make_async_copy(loaded, loaded, load_sem).wait()
    discount = jnp.broadcast_to(1.0 - 1.0 / horizon_ref[...], shape)
    s = jnp.zeros(shape, jnp.float32)
    p = jnp.ones(shape, jnp.float32)
    zero = jnp.zeros(shape, jnp.float32)
    s1, p1, s2, sp, p2 = zero, zero, zero, zero, zero
    for k in reversed(range(chunk)):
        r = rewards[k]
        f = jnp.where(dones[k] == 0, discount, 0.0)
        s = r + f * s
        p = f * p
        s_buf[k] = s
        p_buf[k] = p
        s1 = s1 + s
        p1 = p1 + p
        s2 = s2 + s * s
        sp = sp + s * p
        p2 = p2 + p * p
    full_s, full_p = compose_rows(s, p, row)
    last = row == SUB - 1
    a = jnp.where(last, 0.0, pltpu.roll(full_s, SUB - 1, 0))
    b = jnp.where(last, 1.0, pltpu.roll(full_p, SUB - 1, 0))
    down = lambda value: jnp.sum(value, axis=0, keepdims=True)
    known = jnp.where(t == T - 1, bootstrap_ref[...], jnp.zeros((1, lanes), jnp.float32))
    a = a + b * known
    rest = sp + a * p2
    fold = lambda value: value + pltpu.roll(value, lanes // 2, 1)
    half = lax.broadcasted_iota(jnp.int32, (1, lanes), 1) < lanes // 2
    leading = full_s[0:1] + full_p[0:1] * known
    tbuf[me, 0:1] = jnp.where(half, fold(down(s1 + p1 * a)), fold(down(s2 + a * (sp + rest))))

    @pl.when(t == T - 1)
    def _():
        tbuf[me, 1:2] = leading

    @pl.when(t < T - 1)
    def _():
        tbuf[me, 1:2] = down(p1 * b)
        tbuf[me, 2:3] = down(2.0 * b * rest)
        tbuf[me, 3:4] = down(b * b * p2)
        tbuf[me, 4:5] = jnp.where(t == 0, prior[...], leading)
        tbuf[me, 5:6] = full_p[0:1]

    pl.semaphore_wait(barrier, T * E - 1)
    total = E * sum(rows_sent(T, j) for j in range(T))
    for count in sorted({rows_sent(T, j) for j in range(T)}):
        blocks = [j for j in range(T) if rows_sent(T, j) == count]

        @pl.when(jnp.logical_and(t >= blocks[0], t <= blocks[-1]))
        def _():
            def give(peer, _):
                pltpu.make_async_remote_copy(
                    tbuf.at[me, 0:count], tbuf.at[me, 0:count], send_sem, recv_sem,
                    device_id=peer, device_id_type=pl.DeviceIdType.LOGICAL).start()

            lax.fori_loop(0, me, give, None)
            lax.fori_loop(me + 1, T * E, give, None)
            arrived = measure.at[0:total - count]
            pltpu.make_async_copy(arrived, arrived, recv_sem).wait()
            left = measure.at[0:(T * E - 1) * count]
            pltpu.make_async_copy(left, left, send_sem).wait()

    packed = jnp.zeros((E, lanes), jnp.float32)
    first = jnp.zeros((E, lanes), jnp.float32)
    second = jnp.zeros((E, lanes), jnp.float32)
    x = jnp.zeros((E, lanes), jnp.float32)
    for j in reversed(range(T)):
        part = pl.ds(j * E, E)
        xbuf[j] = x
        packed = packed + tbuf[part, 0]
        if j == T - 1:
            x = tbuf[part, 1]
            continue
        first = first + tbuf[part, 1] * x
        second = second + x * (tbuf[part, 2] + x * tbuf[part, 3])
        if j:
            x = tbuf[part, 4] + tbuf[part, 5] * x
    mine = xbuf[t, pl.ds(e, 1), :]
    prior_ref[0:1] = tbuf[reader(T, E), 4:5]
    prior_ref[1:2] = tbuf[reader(T, E) + 1, 4:5]
    ebuf[0] = packed
    ebuf[1] = first
    ebuf[2] = second
    carry_ref[...] = a + b * mine


def rows_sent(T, block):
    if block == T - 1:
        return 2
    return 6 if block else 5


def reader(T, E):
    return 0


def pick(value, out):
    lane = lax.broadcasted_iota(jnp.int32, out.shape, 1)
    out[...] = jnp.where(lane == 0, value[0], 0.0)


def finish(T, E, rewards, s_buf, p_buf, carry_ref, ebuf, prior_ref, out_rewards, out_returns, out_stats,
           rewards_out, returns_out, stats, sems):
    chunk, _, lanes = rewards.shape
    entries = float(chunk * SUB * T * lanes * E)
    prior_count = entries
    half = lax.broadcasted_iota(jnp.int32, (1, lanes), 1) < lanes // 2
    merged = prior_count + entries
    down = lambda value: jnp.sum(value, axis=0, keepdims=True)
    packed = down(ebuf[0])
    first = (down(ebuf[1]) + jnp.where(half, packed, 0.0)) * (1.0 / entries)
    second = (down(ebuf[2]) + jnp.where(half, 0.0, packed)) * (1.0 / merged)
    across = lambda value: jnp.sum(value, axis=1, keepdims=True)
    average = across(first)
    delta = across(first - prior_ref[0:1])
    squares = across(second + prior_ref[1:2] * (prior_count / merged))
    new_mean = average - delta * (prior_count / merged)
    variance = (squares - average * average * (entries / merged)
                + delta * delta * (prior_count / merged * (entries / merged)))
    inverse = jnp.broadcast_to(lax.rsqrt(variance + 1e-08), (SUB, lanes))

    def send(source, target, rank):
        for i in range(SUB):
            pltpu.make_async_copy(source.at[:, i], target.at[i], sems.at[rank]).start()

    y = carry_ref[...] * inverse
    for k in range(chunk):
        returns_out[k] = s_buf[k] * inverse + p_buf[k] * y
    send(returns_out, out_returns, 0)
    for k in range(chunk):
        rewards_out[k] = rewards[k] * inverse
    send(rewards_out, out_rewards, 1)
    stats[0] = new_mean[0, 0]
    stats[1] = variance[0, 0]
    last = pltpu.make_async_copy(stats, out_stats, sems.at[2])
    last.start()
    pltpu.make_async_copy(returns_out, returns_out, sems.at[0]).wait()
    pltpu.make_async_copy(rewards_out, rewards_out, sems.at[1]).wait()
    last.wait()


def local(T, E, rewards, dones, horizon, bootstrap, prior_mean, prior_var):
    rows, lanes = rewards.shape
    split = (SUB, rows // SUB, lanes)
    vmem = pl.BlockSpec(memory_space=pltpu.VMEM)
    hbm = pl.BlockSpec(memory_space=pltpu.HBM)
    steps = (rows // SUB, SUB, lanes)
    shapes = (steps, steps, steps, (SUB, lanes), (3, E, lanes), (2, lanes))
    exchange = pl.pallas_call(
        functools.partial(kernel, T, E),
        out_shape=tuple(pltpu.VMEM(shape, jnp.float32) for shape in shapes),
        in_specs=[hbm] * 4 + [vmem],
        out_specs=(vmem,) * 6,
        scratch_shapes=[
            pltpu.VMEM(steps, jnp.int32),
            pltpu.VMEM((1, lanes), jnp.float32),
            pltpu.VMEM((1, lanes), jnp.float32),
            pltpu.VMEM((T * E, ROWS, lanes), jnp.float32),
            pltpu.VMEM((T, E, lanes), jnp.float32),
            pltpu.VMEM((max(T * E * ROWS, 2 * rows + 2), lanes), jnp.float32),
            pltpu.SemaphoreType.DMA,
            pltpu.SemaphoreType.DMA,
            pltpu.SemaphoreType.DMA,
        ],
        compiler_params=pltpu.CompilerParams(collective_id=0, has_side_effects=True),
    )
    smem = pl.BlockSpec(memory_space=pltpu.SMEM)
    alone = pl.pallas_call(
        pick, out_shape=jax.ShapeDtypeStruct((1, lanes), jnp.float32), in_specs=[smem], out_specs=vmem)
    me = lax.axis_index("tm") * E + lax.axis_index("env")
    prior = lax.switch(
        jnp.clip(me - reader(T, E) + 1, 0, 3),
        (lambda *_: jnp.zeros((1, lanes), jnp.float32), lambda mean, _: alone(mean), lambda _, var: alone(var),
         lambda *_: jnp.zeros((1, lanes), jnp.float32)), prior_mean, prior_var)
    between = exchange(rewards.reshape(split), dones.reshape(split), horizon.reshape(1, lanes), bootstrap.reshape(1, lanes), prior)
    scaled_rewards, scaled_returns, stats = pl.pallas_call(
        functools.partial(finish, T, E),
        out_shape=(jax.ShapeDtypeStruct(split, jnp.float32),
                   jax.ShapeDtypeStruct(split, jnp.float32),
                   jax.ShapeDtypeStruct((2,), jnp.float32)),
        in_specs=[vmem] * 6,
        out_specs=(hbm, hbm, hbm),
        scratch_shapes=[
            pltpu.VMEM(steps, jnp.float32),
            pltpu.VMEM(steps, jnp.float32),
            pltpu.SMEM((2,), jnp.float32),
            pltpu.SemaphoreType.DMA((3,)),
        ],
        compiler_params=pltpu.CompilerParams(vmem_limit_bytes=4 * 2**20),
    )(*between)
    return scaled_rewards.reshape(rows, lanes), scaled_returns.reshape(rows, lanes), stats


def solution(mesh):
    T, E = mesh.shape["tm"], mesh.shape["env"]
    return jax.shard_map(
        functools.partial(local, T, E),
        mesh=mesh,
        in_specs=(P("tm", "env"), P("tm", "env"), P("env"), P("env"), P(), P()),
        out_specs=(P("tm", "env"), P("tm", "env"), P()),
        check_vma=False,
    )
```

```python
import functools

import jax
import jax.numpy as jnp
from jax import lax
from jax.experimental import pallas as pl
from jax.experimental.pallas import tpu as pltpu
from jax.sharding import PartitionSpec as P

SUB = 8
ROWS = 8
FIRST = 2


def compose_rows(summed, product, row):
    step = 1
    while step < SUB:
        inside = row < SUB - step
        later_sum = jnp.where(inside, pltpu.roll(summed, SUB - step, 0), 0.0)
        later_product = jnp.where(inside, pltpu.roll(product, SUB - step, 0), 1.0)
        summed = summed + product * later_sum
        product = product * later_product
        step *= 2
    return summed, product


def kernel(T, E, rewards_hbm, dones_hbm, horizon_hbm, bootstrap_hbm, prior,
           rewards, s_buf, p_buf, carry_ref, ebuf, prior_ref,
           dones, horizon_ref, bootstrap_ref, tbuf, xbuf, measure,
           load_sem, send_sem, recv_sem):
    t = lax.axis_index("tm")
    e = lax.axis_index("env")
    me = t * E + e
    peers = [k + jnp.where(k >= me, 1, 0) for k in range(T * E - 1)]
    chunk, _, lanes = rewards.shape
    pltpu.make_async_copy(horizon_hbm, horizon_ref, load_sem).start()
    pltpu.make_async_copy(bootstrap_hbm, bootstrap_ref, load_sem).start()
    for source, target in ((rewards_hbm, rewards), (dones_hbm, dones)):
        for i in range(SUB):
            pltpu.make_async_copy(source.at[i], target.at[:, i], load_sem).start()
    barrier = pltpu.get_barrier_semaphore()
    def greet(peer):
        pl.semaphore_signal(barrier, inc=1, device_id=peer, device_id_type=pl.DeviceIdType.LOGICAL)

    lax.fori_loop(0, T * E - 1 - me, lambda i, _: greet(T * E - 1 - i), None)
    lax.fori_loop(0, me, lambda i, _: greet(me - 1 - i), None)
    shape = (SUB, lanes)
    row = lax.broadcasted_iota(jnp.int32, shape, 0)
    @pl.when(me < FIRST)
    def _():
        pl.semaphore_wait(barrier, T * E - 1)

    loaded = measure.at[0:2 * chunk * SUB + 2]
    pltpu.make_async_copy(loaded, loaded, load_sem).wait()
    discount = jnp.broadcast_to(1.0 - 1.0 / horizon_ref[...], shape)
    s = jnp.zeros(shape, jnp.float32)
    p = jnp.ones(shape, jnp.float32)
    zero = jnp.zeros(shape, jnp.float32)
    s1, p1, s2, sp, p2 = zero, zero, zero, zero, zero
    for k in reversed(range(chunk)):
        r = rewards[k]
        f = jnp.where(dones[k] == 0, discount, 0.0)
        s = r + f * s
        p = f * p
        s_buf[k] = s
        p_buf[k] = p
        s1 = s1 + s
        p1 = p1 + p
        s2 = s2 + s * s
        sp = sp + s * p
        p2 = p2 + p * p
    full_s, full_p = compose_rows(s, p, row)
    last = row == SUB - 1
    a = jnp.where(last, 0.0, pltpu.roll(full_s, SUB - 1, 0))
    b = jnp.where(last, 1.0, pltpu.roll(full_p, SUB - 1, 0))
    down = lambda value: jnp.sum(value, axis=0, keepdims=True)
    known = jnp.where(t == T - 1, bootstrap_ref[...], jnp.zeros((1, lanes), jnp.float32))
    a = a + b * known
    rest = sp + a * p2
    fold = lambda value: value + pltpu.roll(value, lanes // 2, 1)
    half = lax.broadcasted_iota(jnp.int32, (1, lanes), 1) < lanes // 2
    leading = full_s[0:1] + full_p[0:1] * known
    tbuf[me, 0:1] = jnp.where(half, fold(down(s1 + p1 * a)), fold(down(s2 + a * (sp + rest))))

    @pl.when(t == T - 1)
    def _():
        tbuf[me, 1:2] = leading

    @pl.when(t < T - 1)
    def _():
        tbuf[me, 1:2] = down(p1 * b)
        tbuf[me, 2:3] = down(2.0 * b * rest)
        tbuf[me, 3:4] = down(b * b * p2)
        tbuf[me, 4:5] = jnp.where(t == 0, prior[...], leading)
        tbuf[me, 5:6] = full_p[0:1]


    @pl.when(me >= FIRST)
    def _():
        pl.semaphore_wait(barrier, T * E - 1)

    total = E * sum(rows_sent(T, j) for j in range(T))
    for count in sorted({rows_sent(T, j) for j in range(T)}):
        blocks = [j for j in range(T) if rows_sent(T, j) == count]

        @pl.when(jnp.logical_and(t >= blocks[0], t <= blocks[-1]))
        def _():
            def give(peer, _):
                pltpu.make_async_remote_copy(
                    tbuf.at[me, 0:count], tbuf.at[me, 0:count], send_sem, recv_sem,
                    device_id=peer, device_id_type=pl.DeviceIdType.LOGICAL).start()

            lax.fori_loop(0, me, give, None)
            lax.fori_loop(me + 1, T * E, give, None)
            arrived = measure.at[0:total - count]
            pltpu.make_async_copy(arrived, arrived, recv_sem).wait()
            left = measure.at[0:(T * E - 1) * count]
            pltpu.make_async_copy(left, left, send_sem).wait()

    packed = jnp.zeros((E, lanes), jnp.float32)
    first = jnp.zeros((E, lanes), jnp.float32)
    second = jnp.zeros((E, lanes), jnp.float32)
    x = jnp.zeros((E, lanes), jnp.float32)
    for j in reversed(range(T)):
        part = pl.ds(j * E, E)
        xbuf[j] = x
        packed = packed + tbuf[part, 0]
        if j == T - 1:
            x = tbuf[part, 1]
            continue
        first = first + tbuf[part, 1] * x
        second = second + x * (tbuf[part, 2] + x * tbuf[part, 3])
        if j:
            x = tbuf[part, 4] + tbuf[part, 5] * x
    mine = xbuf[t, pl.ds(e, 1), :]
    prior_ref[0:1] = tbuf[reader(T, E), 4:5]
    prior_ref[1:2] = tbuf[reader(T, E) + 1, 4:5]
    ebuf[0] = packed
    ebuf[1] = first
    ebuf[2] = second
    carry_ref[...] = a + b * mine


def rows_sent(T, block):
    if block == T - 1:
        return 2
    return 6 if block else 5


def reader(T, E):
    return 0


def pick(value, out):
    lane = lax.broadcasted_iota(jnp.int32, out.shape, 1)
    out[...] = jnp.where(lane == 0, value[0], 0.0)


def finish(T, E, rewards, s_buf, p_buf, carry_ref, ebuf, prior_ref, out_rewards, out_returns, out_stats,
           rewards_out, returns_out, stats, sems):
    chunk, _, lanes = rewards.shape
    entries = float(chunk * SUB * T * lanes * E)
    prior_count = entries
    half = lax.broadcasted_iota(jnp.int32, (1, lanes), 1) < lanes // 2
    merged = prior_count + entries
    down = lambda value: jnp.sum(value, axis=0, keepdims=True)
    packed = down(ebuf[0])
    first = (down(ebuf[1]) + jnp.where(half, packed, 0.0)) * (1.0 / entries)
    second = (down(ebuf[2]) + jnp.where(half, 0.0, packed)) * (1.0 / merged)
    across = lambda value: jnp.sum(value, axis=1, keepdims=True)
    average = across(first)
    delta = across(first - prior_ref[0:1])
    squares = across(second + prior_ref[1:2] * (prior_count / merged))
    new_mean = average - delta * (prior_count / merged)
    variance = (squares - average * average * (entries / merged)
                + delta * delta * (prior_count / merged * (entries / merged)))
    inverse = jnp.broadcast_to(lax.rsqrt(variance + 1e-08), (SUB, lanes))

    def send(source, target, rank):
        for i in range(SUB):
            pltpu.make_async_copy(source.at[:, i], target.at[i], sems.at[rank]).start()

    y = carry_ref[...] * inverse
    for k in range(chunk):
        returns_out[k] = s_buf[k] * inverse + p_buf[k] * y
    send(returns_out, out_returns, 0)
    for k in range(chunk):
        rewards_out[k] = rewards[k] * inverse
    send(rewards_out, out_rewards, 1)
    stats[0] = new_mean[0, 0]
    stats[1] = variance[0, 0]
    last = pltpu.make_async_copy(stats, out_stats, sems.at[2])
    last.start()
    pltpu.make_async_copy(returns_out, returns_out, sems.at[0]).wait()
    pltpu.make_async_copy(rewards_out, rewards_out, sems.at[1]).wait()
    last.wait()


def local(T, E, rewards, dones, horizon, bootstrap, prior_mean, prior_var):
    rows, lanes = rewards.shape
    split = (SUB, rows // SUB, lanes)
    vmem = pl.BlockSpec(memory_space=pltpu.VMEM)
    hbm = pl.BlockSpec(memory_space=pltpu.HBM)
    steps = (rows // SUB, SUB, lanes)
    shapes = (steps, steps, steps, (SUB, lanes), (3, E, lanes), (2, lanes))
    exchange = pl.pallas_call(
        functools.partial(kernel, T, E),
        out_shape=tuple(pltpu.VMEM(shape, jnp.float32) for shape in shapes),
        in_specs=[hbm] * 4 + [vmem],
        out_specs=(vmem,) * 6,
        scratch_shapes=[
            pltpu.VMEM(steps, jnp.int32),
            pltpu.VMEM((1, lanes), jnp.float32),
            pltpu.VMEM((1, lanes), jnp.float32),
            pltpu.VMEM((T * E, ROWS, lanes), jnp.float32),
            pltpu.VMEM((T, E, lanes), jnp.float32),
            pltpu.VMEM((max(T * E * ROWS, 2 * rows + 2), lanes), jnp.float32),
            pltpu.SemaphoreType.DMA,
            pltpu.SemaphoreType.DMA,
            pltpu.SemaphoreType.DMA,
        ],
        compiler_params=pltpu.CompilerParams(collective_id=0, has_side_effects=True),
    )
    smem = pl.BlockSpec(memory_space=pltpu.SMEM)
    alone = pl.pallas_call(
        pick, out_shape=jax.ShapeDtypeStruct((1, lanes), jnp.float32), in_specs=[smem], out_specs=vmem)
    me = lax.axis_index("tm") * E + lax.axis_index("env")
    prior = lax.switch(
        jnp.clip(me - reader(T, E) + 1, 0, 3),
        (lambda *_: jnp.zeros((1, lanes), jnp.float32), lambda mean, _: alone(mean), lambda _, var: alone(var),
         lambda *_: jnp.zeros((1, lanes), jnp.float32)), prior_mean, prior_var)
    between = exchange(rewards.reshape(split), dones.reshape(split), horizon.reshape(1, lanes), bootstrap.reshape(1, lanes), prior)
    scaled_rewards, scaled_returns, stats = pl.pallas_call(
        functools.partial(finish, T, E),
        out_shape=(jax.ShapeDtypeStruct(split, jnp.float32),
                   jax.ShapeDtypeStruct(split, jnp.float32),
                   jax.ShapeDtypeStruct((2,), jnp.float32)),
        in_specs=[vmem] * 6,
        out_specs=(hbm, hbm, hbm),
        scratch_shapes=[
            pltpu.VMEM(steps, jnp.float32),
            pltpu.VMEM(steps, jnp.float32),
            pltpu.SMEM((2,), jnp.float32),
            pltpu.SemaphoreType.DMA((3,)),
        ],
        compiler_params=pltpu.CompilerParams(vmem_limit_bytes=4 * 2**20),
    )(*between)
    return scaled_rewards.reshape(rows, lanes), scaled_returns.reshape(rows, lanes), stats


def solution(mesh):
    T, E = mesh.shape["tm"], mesh.shape["env"]
    return jax.shard_map(
        functools.partial(local, T, E),
        mesh=mesh,
        in_specs=(P("tm", "env"), P("tm", "env"), P("env"), P("env"), P(), P()),
        out_specs=(P("tm", "env"), P("tm", "env"), P()),
        check_vma=False,
    )
```

```python
import functools

import jax
import jax.numpy as jnp
from jax import lax
from jax.experimental import pallas as pl
from jax.experimental.pallas import tpu as pltpu
from jax.sharding import PartitionSpec as P

SUB = 8
ROWS = 8
FIRST = 2


def compose_rows(summed, product, row):
    step = 1
    while step < SUB:
        inside = row < SUB - step
        later_sum = jnp.where(inside, pltpu.roll(summed, SUB - step, 0), 0.0)
        later_product = jnp.where(inside, pltpu.roll(product, SUB - step, 0), 1.0)
        summed = summed + product * later_sum
        product = product * later_product
        step *= 2
    return summed, product


def kernel(T, E, rewards_hbm, dones_hbm, horizon_hbm, bootstrap_hbm, prior,
           rewards, s_buf, p_buf, carry_ref, ebuf, prior_ref,
           dones, horizon_ref, bootstrap_ref, tbuf, xbuf, measure,
           load_sem, send_sem, recv_sem):
    t = lax.axis_index("tm")
    e = lax.axis_index("env")
    me = t * E + e
    peers = [k + jnp.where(k >= me, 1, 0) for k in range(T * E - 1)]
    chunk, _, lanes = rewards.shape
    pltpu.make_async_copy(horizon_hbm, horizon_ref, load_sem).start()
    pltpu.make_async_copy(bootstrap_hbm, bootstrap_ref, load_sem).start()
    for source, target in ((rewards_hbm, rewards), (dones_hbm, dones)):
        for i in range(SUB):
            pltpu.make_async_copy(source.at[i], target.at[:, i], load_sem).start()
    barrier = pltpu.get_barrier_semaphore()
    def greet(peer):
        pl.semaphore_signal(barrier, inc=1, device_id=peer, device_id_type=pl.DeviceIdType.LOGICAL)

    late = 2 * t >= T
    origin, turn = jnp.where(late, 0, T * E - 1), jnp.where(late, 1, -1)
    before = jnp.where(late, me, T * E - 1 - me)
    lax.fori_loop(0, before, lambda i, _: greet(origin + turn * i), None)
    lax.fori_loop(before + 1, T * E, lambda i, _: greet(origin + turn * i), None)
    shape = (SUB, lanes)
    row = lax.broadcasted_iota(jnp.int32, shape, 0)
    @pl.when(me < FIRST)
    def _():
        pl.semaphore_wait(barrier, T * E - 1)

    loaded = measure.at[0:2 * chunk * SUB + 2]
    pltpu.make_async_copy(loaded, loaded, load_sem).wait()
    discount = jnp.broadcast_to(1.0 - 1.0 / horizon_ref[...], shape)
    s = jnp.zeros(shape, jnp.float32)
    p = jnp.ones(shape, jnp.float32)
    zero = jnp.zeros(shape, jnp.float32)
    s1, p1, s2, sp, p2 = zero, zero, zero, zero, zero
    for k in reversed(range(chunk)):
        r = rewards[k]
        f = jnp.where(dones[k] == 0, discount, 0.0)
        s = r + f * s
        p = f * p
        s_buf[k] = s
        p_buf[k] = p
        s1 = s1 + s
        p1 = p1 + p
        s2 = s2 + s * s
        sp = sp + s * p
        p2 = p2 + p * p
    full_s, full_p = compose_rows(s, p, row)
    last = row == SUB - 1
    a = jnp.where(last, 0.0, pltpu.roll(full_s, SUB - 1, 0))
    b = jnp.where(last, 1.0, pltpu.roll(full_p, SUB - 1, 0))
    down = lambda value: jnp.sum(value, axis=0, keepdims=True)
    known = jnp.where(t == T - 1, bootstrap_ref[...], jnp.zeros((1, lanes), jnp.float32))
    a = a + b * known
    rest = sp + a * p2
    leading = full_s[0:1] + full_p[0:1] * known
    first = down(s1 + p1 * a)
    second = down(s2 + a * (sp + rest))

    @pl.when(t == T - 1)
    def _():
        tbuf[me, 0:1] = first
        tbuf[me, 1:2] = second
        tbuf[me, 2:3] = leading

    @pl.when(t < T - 1)
    def _():
        fold = lambda value: value + pltpu.roll(value, lanes // 2, 1)
        half = lax.broadcasted_iota(jnp.int32, (1, lanes), 1) < lanes // 2
        tbuf[me, 0:1] = jnp.where(half, fold(first), fold(second))
        tbuf[me, 1:2] = down(p1 * b)
        tbuf[me, 2:3] = down(2.0 * b * rest)
        tbuf[me, 3:4] = down(b * b * p2)
        tbuf[me, 4:5] = jnp.where(t == 0, prior[...], leading)
        tbuf[me, 5:6] = full_p[0:1]


    @pl.when(me >= FIRST)
    def _():
        pl.semaphore_wait(barrier, T * E - 1)

    total = E * sum(rows_sent(T, j) for j in range(T))
    for count in sorted({rows_sent(T, j) for j in range(T)}):
        blocks = [j for j in range(T) if rows_sent(T, j) == count]

        @pl.when(jnp.logical_and(t >= blocks[0], t <= blocks[-1]))
        def _():
            def give(peer, _):
                pltpu.make_async_remote_copy(
                    tbuf.at[me, 0:count], tbuf.at[me, 0:count], send_sem, recv_sem,
                    device_id=peer, device_id_type=pl.DeviceIdType.LOGICAL).start()

            lax.fori_loop(0, me, give, None)
            lax.fori_loop(me + 1, T * E, give, None)
            arrived = measure.at[0:total - count]
            pltpu.make_async_copy(arrived, arrived, recv_sem).wait()
            left = measure.at[0:(T * E - 1) * count]
            pltpu.make_async_copy(left, left, send_sem).wait()

    packed = jnp.zeros((E, lanes), jnp.float32)
    first = jnp.zeros((E, lanes), jnp.float32)
    second = jnp.zeros((E, lanes), jnp.float32)
    x = jnp.zeros((E, lanes), jnp.float32)
    for j in reversed(range(T)):
        part = pl.ds(j * E, E)
        xbuf[j] = x
        if j == T - 1:
            first = first + tbuf[part, 0]
            second = second + tbuf[part, 1]
            x = tbuf[part, 2]
            continue
        packed = packed + tbuf[part, 0]
        first = first + tbuf[part, 1] * x
        second = second + x * (tbuf[part, 2] + x * tbuf[part, 3])
        if j:
            x = tbuf[part, 4] + tbuf[part, 5] * x
    mine = xbuf[t, pl.ds(e, 1), :]
    prior_ref[0:1] = tbuf[reader(T, E), 4:5]
    prior_ref[1:2] = tbuf[reader(T, E) + 1, 4:5]
    ebuf[0] = packed
    ebuf[1] = first
    ebuf[2] = second
    carry_ref[...] = a + b * mine


def rows_sent(T, block):
    if block == T - 1:
        return 3
    return 6 if block else 5


def reader(T, E):
    return 0


def pick(value, out):
    lane = lax.broadcasted_iota(jnp.int32, out.shape, 1)
    out[...] = jnp.where(lane == 0, value[0], 0.0)


def finish(T, E, rewards, s_buf, p_buf, carry_ref, ebuf, prior_ref, out_rewards, out_returns, out_stats,
           both_out, stats, sems):
    chunk, _, lanes = rewards.shape
    rewards_out, returns_out = both_out.at[0], both_out.at[1]
    entries = float(chunk * SUB * T * lanes * E)
    prior_count = entries
    half = lax.broadcasted_iota(jnp.int32, (1, lanes), 1) < lanes // 2
    merged = prior_count + entries
    down = lambda value: jnp.sum(value, axis=0, keepdims=True)
    packed = down(ebuf[0])
    first = (down(ebuf[1]) + jnp.where(half, packed, 0.0)) * (1.0 / entries)
    second = (down(ebuf[2]) + jnp.where(half, 0.0, packed)) * (1.0 / merged)
    across = lambda value: jnp.sum(value, axis=1, keepdims=True)
    average = across(first)
    delta = across(first - prior_ref[0:1])
    squares = across(second + prior_ref[1:2] * (prior_count / merged))
    new_mean = average - delta * (prior_count / merged)
    variance = (squares - average * average * (entries / merged)
                + delta * delta * (prior_count / merged * (entries / merged)))
    inverse = jnp.broadcast_to(lax.rsqrt(variance + 1e-08), (SUB, lanes))

    def send(source, target, rank):
        for i in range(SUB):
            pltpu.make_async_copy(source.at[:, i], target.at[i], sems.at[rank]).start()

    y = carry_ref[...] * inverse
    for k in range(chunk):
        returns_out[k] = s_buf[k] * inverse + p_buf[k] * y
    send(returns_out, out_returns, 0)
    for k in range(chunk):
        rewards_out[k] = rewards[k] * inverse
    send(rewards_out, out_rewards, 0)
    stats[0] = new_mean[0, 0]
    stats[1] = variance[0, 0]
    last = pltpu.make_async_copy(stats, out_stats, sems.at[1])
    last.start()
    pltpu.make_async_copy(both_out, both_out, sems.at[0]).wait()
    last.wait()


def local(T, E, rewards, dones, horizon, bootstrap, prior_mean, prior_var):
    rows, lanes = rewards.shape
    split = (SUB, rows // SUB, lanes)
    vmem = pl.BlockSpec(memory_space=pltpu.VMEM)
    hbm = pl.BlockSpec(memory_space=pltpu.HBM)
    steps = (rows // SUB, SUB, lanes)
    shapes = (steps, steps, steps, (SUB, lanes), (3, E, lanes), (2, lanes))
    exchange = pl.pallas_call(
        functools.partial(kernel, T, E),
        out_shape=tuple(pltpu.VMEM(shape, jnp.float32) for shape in shapes),
        in_specs=[hbm] * 4 + [vmem],
        out_specs=(vmem,) * 6,
        scratch_shapes=[
            pltpu.VMEM(steps, jnp.int32),
            pltpu.VMEM((1, lanes), jnp.float32),
            pltpu.VMEM((1, lanes), jnp.float32),
            pltpu.VMEM((T * E, ROWS, lanes), jnp.float32),
            pltpu.VMEM((T, E, lanes), jnp.float32),
            pltpu.VMEM((max(T * E * ROWS, 2 * rows + 2), lanes), jnp.float32),
            pltpu.SemaphoreType.DMA,
            pltpu.SemaphoreType.DMA,
            pltpu.SemaphoreType.DMA,
        ],
        compiler_params=pltpu.CompilerParams(collective_id=0, has_side_effects=True),
    )
    smem = pl.BlockSpec(memory_space=pltpu.SMEM)
    alone = pl.pallas_call(
        pick, out_shape=jax.ShapeDtypeStruct((1, lanes), jnp.float32), in_specs=[smem], out_specs=vmem)
    me = lax.axis_index("tm") * E + lax.axis_index("env")
    prior = lax.switch(
        jnp.clip(me - reader(T, E) + 1, 0, 3),
        (lambda *_: jnp.zeros((1, lanes), jnp.float32), lambda mean, _: alone(mean), lambda _, var: alone(var),
         lambda *_: jnp.zeros((1, lanes), jnp.float32)), prior_mean, prior_var)
    between = exchange(rewards.reshape(split), dones.reshape(split), horizon.reshape(1, lanes), bootstrap.reshape(1, lanes), prior)
    scaled_rewards, scaled_returns, stats = pl.pallas_call(
        functools.partial(finish, T, E),
        out_shape=(jax.ShapeDtypeStruct(split, jnp.float32),
                   jax.ShapeDtypeStruct(split, jnp.float32),
                   jax.ShapeDtypeStruct((2,), jnp.float32)),
        in_specs=[vmem] * 6,
        out_specs=(hbm, hbm, hbm),
        scratch_shapes=[
            pltpu.VMEM((2,) + steps, jnp.float32),
            pltpu.SMEM((2,), jnp.float32),
            pltpu.SemaphoreType.DMA((2,)),
        ],
        compiler_params=pltpu.CompilerParams(vmem_limit_bytes=4 * 2**20),
    )(*between)
    return scaled_rewards.reshape(rows, lanes), scaled_returns.reshape(rows, lanes), stats


def solution(mesh):
    T, E = mesh.shape["tm"], mesh.shape["env"]
    return jax.shard_map(
        functools.partial(local, T, E),
        mesh=mesh,
        in_specs=(P("tm", "env"), P("tm", "env"), P("env"), P("env"), P(), P()),
        out_specs=(P("tm", "env"), P("tm", "env"), P()),
        check_vma=False,
    )
```

```python
import functools

import jax
import jax.numpy as jnp
from jax import lax
from jax.experimental import pallas as pl
from jax.experimental.pallas import tpu as pltpu
from jax.sharding import PartitionSpec as P

SUB = 8
ROWS = 8
FIRST = 2


def compose_rows(summed, product, row):
    step = 1
    while step < SUB:
        inside = row < SUB - step
        later_sum = jnp.where(inside, pltpu.roll(summed, SUB - step, 0), 0.0)
        later_product = jnp.where(inside, pltpu.roll(product, SUB - step, 0), 1.0)
        summed = summed + product * later_sum
        product = product * later_product
        step *= 2
    return summed, product


def kernel(T, E, rewards_hbm, dones_hbm, horizon_hbm, bootstrap_hbm, prior,
           rewards, s_buf, p_buf, carry_ref, ebuf, prior_ref,
           dones, horizon_ref, bootstrap_ref, tbuf, xbuf, measure,
           load_sem, send_sem, recv_sem):
    t = lax.axis_index("tm")
    e = lax.axis_index("env")
    me = t * E + e
    peers = [k + jnp.where(k >= me, 1, 0) for k in range(T * E - 1)]
    chunk, _, lanes = rewards.shape
    pltpu.make_async_copy(horizon_hbm, horizon_ref, load_sem).start()
    pltpu.make_async_copy(bootstrap_hbm, bootstrap_ref, load_sem).start()
    for source, target in ((rewards_hbm, rewards), (dones_hbm, dones)):
        for i in range(SUB):
            pltpu.make_async_copy(source.at[i], target.at[:, i], load_sem).start()
    barrier = pltpu.get_barrier_semaphore()
    def greet(peer):
        pl.semaphore_signal(barrier, inc=1, device_id=peer, device_id_type=pl.DeviceIdType.LOGICAL)

    late = 2 * t >= T
    origin, turn = jnp.where(late, 0, T * E - 1), jnp.where(late, 1, -1)
    before = jnp.where(late, me, T * E - 1 - me)
    lax.fori_loop(0, before, lambda i, _: greet(origin + turn * i), None)
    lax.fori_loop(before + 1, T * E, lambda i, _: greet(origin + turn * i), None)
    shape = (SUB, lanes)
    row = lax.broadcasted_iota(jnp.int32, shape, 0)
    @pl.when(me < FIRST)
    def _():
        pl.semaphore_wait(barrier, T * E - 1)

    loaded = measure.at[0:2 * chunk * SUB + 2]
    pltpu.make_async_copy(loaded, loaded, load_sem).wait()
    discount = jnp.broadcast_to(1.0 - 1.0 / horizon_ref[...], shape)
    s = jnp.zeros(shape, jnp.float32)
    p = jnp.ones(shape, jnp.float32)
    zero = jnp.zeros(shape, jnp.float32)
    s1, p1, s2, sp, p2 = zero, zero, zero, zero, zero
    for k in reversed(range(chunk)):
        r = rewards[k]
        f = jnp.where(dones[k] == 0, discount, 0.0)
        s = r + f * s
        p = f * p
        s_buf[k] = s
        p_buf[k] = p
        s1 = s1 + s
        p1 = p1 + p
        s2 = s2 + s * s
        sp = sp + s * p
        p2 = p2 + p * p
    full_s, full_p = compose_rows(s, p, row)
    last = row == SUB - 1
    a = jnp.where(last, 0.0, pltpu.roll(full_s, SUB - 1, 0))
    b = jnp.where(last, 1.0, pltpu.roll(full_p, SUB - 1, 0))
    down = lambda value: jnp.sum(value, axis=0, keepdims=True)
    known = jnp.where(t == T - 1, bootstrap_ref[...], jnp.zeros((1, lanes), jnp.float32))
    a = a + b * known
    rest = sp + a * p2
    leading = full_s[0:1] + full_p[0:1] * known
    first = down(s1 + p1 * a)
    second = down(s2 + a * (sp + rest))

    @pl.when(t == T - 1)
    def _():
        tbuf[me, 0:1] = first
        tbuf[me, 1:2] = second
        tbuf[me, 2:3] = leading

    @pl.when(t < T - 1)
    def _():
        fold = lambda value: value + pltpu.roll(value, lanes // 2, 1)
        half = lax.broadcasted_iota(jnp.int32, (1, lanes), 1) < lanes // 2
        tbuf[me, 0:1] = jnp.where(half, fold(first), fold(second))
        tbuf[me, 1:2] = down(p1 * b)
        tbuf[me, 2:3] = down(2.0 * b * rest)
        tbuf[me, 3:4] = down(b * b * p2)
        tbuf[me, 4:5] = jnp.where(t == 0, prior[...], leading)
        tbuf[me, 5:6] = full_p[0:1]


    @pl.when(me >= FIRST)
    def _():
        pl.semaphore_wait(barrier, T * E - 1)

    total = E * sum(rows_sent(T, j) for j in range(T))
    for count in sorted({rows_sent(T, j) for j in range(T)}):
        blocks = [j for j in range(T) if rows_sent(T, j) == count]

        @pl.when(jnp.logical_and(t >= blocks[0], t <= blocks[-1]))
        def _():
            def give(peer, _):
                pltpu.make_async_remote_copy(
                    tbuf.at[me, 0:count], tbuf.at[me, 0:count], send_sem, recv_sem,
                    device_id=peer, device_id_type=pl.DeviceIdType.LOGICAL).start()

            lax.fori_loop(0, me, give, None)
            lax.fori_loop(me + 1, T * E, give, None)
            left = measure.at[0:(T * E - 1) * count]
            pltpu.make_async_copy(left, left, send_sem).wait()
            arrived = measure.at[0:total - count]
            pltpu.make_async_copy(arrived, arrived, recv_sem).wait()

    packed = jnp.zeros((E, lanes), jnp.float32)
    first = jnp.zeros((E, lanes), jnp.float32)
    second = jnp.zeros((E, lanes), jnp.float32)
    x = jnp.zeros((E, lanes), jnp.float32)
    for j in reversed(range(T)):
        part = pl.ds(j * E, E)
        xbuf[j] = x
        if j == T - 1:
            first = first + tbuf[part, 0]
            second = second + tbuf[part, 1]
            x = tbuf[part, 2]
            continue
        packed = packed + tbuf[part, 0]
        first = first + tbuf[part, 1] * x
        second = second + x * (tbuf[part, 2] + x * tbuf[part, 3])
        if j:
            x = tbuf[part, 4] + tbuf[part, 5] * x
    mine = xbuf[t, pl.ds(e, 1), :]
    prior_ref[0:1] = tbuf[reader(T, E), 4:5]
    prior_ref[1:2] = tbuf[reader(T, E) + 1, 4:5]
    ebuf[0] = packed
    ebuf[1] = first
    ebuf[2] = second
    carry_ref[...] = a + b * mine


def rows_sent(T, block):
    if block == T - 1:
        return 3
    return 6 if block else 5


def reader(T, E):
    return 0


def pick(value, out):
    lane = lax.broadcasted_iota(jnp.int32, out.shape, 1)
    out[...] = jnp.where(lane == 0, value[0], 0.0)


def finish(T, E, rewards, s_buf, p_buf, carry_ref, ebuf, prior_ref, out_rewards, out_returns, out_stats,
           both_out, stats, sems):
    chunk, _, lanes = rewards.shape
    rewards_out, returns_out = both_out.at[0], both_out.at[1]
    entries = float(chunk * SUB * T * lanes * E)
    prior_count = entries
    half = lax.broadcasted_iota(jnp.int32, (1, lanes), 1) < lanes // 2
    merged = prior_count + entries
    down = lambda value: jnp.sum(value, axis=0, keepdims=True)
    packed = down(ebuf[0])
    first = (down(ebuf[1]) + jnp.where(half, packed, 0.0)) * (1.0 / entries)
    second = (down(ebuf[2]) + jnp.where(half, 0.0, packed)) * (1.0 / merged)
    across = lambda value: jnp.sum(value, axis=1, keepdims=True)
    average = across(first)
    delta = across(first - prior_ref[0:1])
    squares = across(second + prior_ref[1:2] * (prior_count / merged))
    new_mean = average - delta * (prior_count / merged)
    variance = (squares - average * average * (entries / merged)
                + delta * delta * (prior_count / merged * (entries / merged)))
    inverse = jnp.broadcast_to(lax.rsqrt(variance + 1e-08), (SUB, lanes))

    def send(source, target, rank):
        for i in range(SUB):
            pltpu.make_async_copy(source.at[:, i], target.at[i], sems.at[rank]).start()

    y = carry_ref[...] * inverse
    for k in range(chunk):
        returns_out[k] = s_buf[k] * inverse + p_buf[k] * y
    send(returns_out, out_returns, 0)
    for k in range(chunk):
        rewards_out[k] = rewards[k] * inverse
    send(rewards_out, out_rewards, 0)
    stats[0] = new_mean[0, 0]
    stats[1] = variance[0, 0]
    last = pltpu.make_async_copy(stats, out_stats, sems.at[1])
    last.start()
    pltpu.make_async_copy(both_out, both_out, sems.at[0]).wait()
    last.wait()


def local(T, E, rewards, dones, horizon, bootstrap, prior_mean, prior_var):
    rows, lanes = rewards.shape
    split = (SUB, rows // SUB, lanes)
    vmem = pl.BlockSpec(memory_space=pltpu.VMEM)
    hbm = pl.BlockSpec(memory_space=pltpu.HBM)
    steps = (rows // SUB, SUB, lanes)
    shapes = (steps, steps, steps, (SUB, lanes), (3, E, lanes), (2, lanes))
    exchange = pl.pallas_call(
        functools.partial(kernel, T, E),
        out_shape=tuple(pltpu.VMEM(shape, jnp.float32) for shape in shapes),
        in_specs=[hbm] * 4 + [vmem],
        out_specs=(vmem,) * 6,
        scratch_shapes=[
            pltpu.VMEM(steps, jnp.int32),
            pltpu.VMEM((1, lanes), jnp.float32),
            pltpu.VMEM((1, lanes), jnp.float32),
            pltpu.VMEM((T * E, ROWS, lanes), jnp.float32),
            pltpu.VMEM((T, E, lanes), jnp.float32),
            pltpu.VMEM((max(T * E * ROWS, 2 * rows + 2), lanes), jnp.float32),
            pltpu.SemaphoreType.DMA,
            pltpu.SemaphoreType.DMA,
            pltpu.SemaphoreType.DMA,
        ],
        compiler_params=pltpu.CompilerParams(collective_id=0, has_side_effects=True),
    )
    smem = pl.BlockSpec(memory_space=pltpu.SMEM)
    alone = pl.pallas_call(
        pick, out_shape=jax.ShapeDtypeStruct((1, lanes), jnp.float32), in_specs=[smem], out_specs=vmem)
    me = lax.axis_index("tm") * E + lax.axis_index("env")
    prior = lax.switch(
        jnp.clip(me - reader(T, E) + 1, 0, 3),
        (lambda *_: jnp.zeros((1, lanes), jnp.float32), lambda mean, _: alone(mean), lambda _, var: alone(var),
         lambda *_: jnp.zeros((1, lanes), jnp.float32)), prior_mean, prior_var)
    between = exchange(rewards.reshape(split), dones.reshape(split), horizon.reshape(1, lanes), bootstrap.reshape(1, lanes), prior)
    scaled_rewards, scaled_returns, stats = pl.pallas_call(
        functools.partial(finish, T, E),
        out_shape=(jax.ShapeDtypeStruct(split, jnp.float32),
                   jax.ShapeDtypeStruct(split, jnp.float32),
                   jax.ShapeDtypeStruct((2,), jnp.float32)),
        in_specs=[vmem] * 6,
        out_specs=(hbm, hbm, hbm),
        scratch_shapes=[
            pltpu.VMEM((2,) + steps, jnp.float32),
            pltpu.SMEM((2,), jnp.float32),
            pltpu.SemaphoreType.DMA((2,)),
        ],
        compiler_params=pltpu.CompilerParams(vmem_limit_bytes=4 * 2**20),
    )(*between)
    return scaled_rewards.reshape(rows, lanes), scaled_returns.reshape(rows, lanes), stats


def solution(mesh):
    T, E = mesh.shape["tm"], mesh.shape["env"]
    return jax.shard_map(
        functools.partial(local, T, E),
        mesh=mesh,
        in_specs=(P("tm", "env"), P("tm", "env"), P("env"), P("env"), P(), P()),
        out_specs=(P("tm", "env"), P("tm", "env"), P()),
        check_vma=False,
    )
```
